8 devices in a mesh: dp: 2 (over y, z), tp: 4 (over x, core).
Axes of the slice: x: 2, y: 2, z: 1, core: 2. Of those that a mesh axis runs over, the one named last changes fastest.
Arguments:
- x: bfloat16 [128, 2048], P('dp'), parts along dimension 0
- k_cache: bfloat16 [128, 1024, 16, 128], P('dp', None, 'tp'), parts along dimension 0
- v_cache: bfloat16 [128, 1024, 16, 128], P('dp', None, 'tp'), parts along dimension 0
- gain_a: bfloat16 [2048], replicated
- wq: bfloat16 [2048, 2048], P(None, 'tp')
- wo: bfloat16 [2048, 2048], P('tp')
- gain_m: bfloat16 [2048], replicated
- w_gate: bfloat16 [2048, 8192], P(None, 'tp')
- w_up: bfloat16 [2048, 8192], P(None, 'tp')
- w_down: bfloat16 [8192, 2048], P('tp')
Outputs:
- output: bfloat16 [128, 2048], P('dp'), parts along dimension 0
There are 2 independent parts. The reference program is written for one: setup_inputs(seed, part) draws one part's arguments, and reference() takes and returns one part's arrays. A program takes and returns all parts, laid end to end along the dimension named above; an argument that names none is the same for every part.
All inputs are finite; a program needn't handle non-finite values.
Results may differ from the reference program's by a relative error of at most 0.017.
Values are sent between devices in bfloat16 or wider.
A program may use at most 2 GiB of HBM per device.

```python
import jax
import jax.numpy as jnp
from jax import lax

BATCH = 64
CACHE = 1024
D = 2048
HEADS = 16
KV_HEADS = 16
HEAD = 128
FF = 8192
THETA = 10000


def setup_inputs(seed: int = 0, part: int = 0) -> dict:
    kx, kc, kw, kn, kq, ko, km, kg, ku, kd = jax.random.split(jax.random.key(seed), 10)
    kx, kc, kw = (jax.random.fold_in(k, part) for k in (kx, kc, kw))

    def weights(key, rows, columns):
        return jax.random.normal(key, (rows, columns), jnp.float32) * rows**-0.5

    drawn = {
        "x": jax.random.normal(kx, (BATCH, D), jnp.float32),
        "k_cache": 2 * jax.random.normal(kc, (BATCH, CACHE, KV_HEADS, HEAD), jnp.float32),
        "v_cache": 4 * jax.random.normal(kw, (BATCH, CACHE, KV_HEADS, HEAD), jnp.float32),
        "gain_a": 1 + 0.1 * jax.random.normal(kn, (D,), jnp.float32),
        "wq": 2 * weights(kq, D, HEADS * HEAD),
        "wo": weights(ko, HEADS * HEAD, D),
        "gain_m": 1 + 0.1 * jax.random.normal(km, (D,), jnp.float32),
        "w_gate": weights(kg, D, FF),
        "w_up": weights(ku, D, FF),
        "w_down": 2 * weights(kd, FF, D),
    }
    return {k: v.astype(jnp.bfloat16) for k, v in drawn.items()}


def normed(x, gain):
    wide = x.astype(jnp.float32)
    scale = lax.rsqrt(jnp.mean(wide * wide, -1, keepdims=True) + 1e-6)
    return (wide * scale * gain.astype(jnp.float32)).astype(jnp.bfloat16)


def turned(t, place, theta):
    half = t.shape[-1] // 2
    angle = place.astype(jnp.float32)[:, None] * theta ** (-jnp.arange(half, dtype=jnp.float32) / half)
    cos, sin = jnp.cos(angle)[:, None], jnp.sin(angle)[:, None]
    a, b = t[..., :half].astype(jnp.float32), t[..., half:].astype(jnp.float32)
    return jnp.concatenate([a * cos - b * sin, b * cos + a * sin], -1).astype(jnp.bfloat16)


def matmul(a, w):
    return jnp.dot(a, w, preferred_element_type=jnp.float32).astype(jnp.bfloat16)


def einsum(form, a, b):
    return jnp.einsum(form, a.astype(jnp.float32), b.astype(jnp.float32))


def seen_by(a, wq, k_cache, v_cache, head, theta):
    batch, cache, kv_heads = k_cache.shape[:3]
    place = jnp.full((batch,), cache - 1)
    q = turned(matmul(a, wq).reshape(batch, -1, head), place, theta).reshape(batch, kv_heads, -1, head)
    scores = einsum("bgsd,bugd->bgsu", q, k_cache) * head**-0.5
    weights = jax.nn.softmax(scores, -1).astype(jnp.bfloat16)
    return einsum("bgsu,bugd->bgsd", weights, v_cache).astype(jnp.bfloat16).reshape(batch, -1)


def hidden_of(b, w_gate, w_up):
    gate = jnp.dot(b, w_gate, preferred_element_type=jnp.float32)
    up = jnp.dot(b, w_up, preferred_element_type=jnp.float32)
    return (jax.nn.silu(gate) * up).astype(jnp.bfloat16)


def reference(x, k_cache, v_cache, gain_a, wq, wo, gain_m, w_gate, w_up, w_down):
    seen = seen_by(normed(x, gain_a), wq, k_cache, v_cache, HEAD, THETA)
    h = (x.astype(jnp.float32) + jnp.dot(seen, wo, preferred_element_type=jnp.float32)).astype(jnp.bfloat16)
    hidden = hidden_of(normed(h, gain_m), w_gate, w_up)
    return (h.astype(jnp.float32) + jnp.dot(hidden, w_down, preferred_element_type=jnp.float32)).astype(jnp.bfloat16)
```

```python
import jax
import jax.numpy as jnp
import numpy as np
from jax import lax
from jax.experimental import pallas as pl
from jax.experimental.pallas import tpu as pltpu
from jax.sharding import PartitionSpec as P

MESH = pl.DeviceIdType.MESH
HEAD = 128
THETA = 10000
ROWS, D, CACHE, HEADS = 64, 2048, 1024, 4
KV = CACHE * HEADS
PAIRS = ROWS // 2
DEPTH = 6
CHUNK = 16
CHUNKS = ROWS // CHUNK
PER = CHUNK // 2
HALF = D // 2
FF = 2048
NCOL = 512
PIECES = D // NCOL
F32, BF16 = jnp.float32, jnp.bfloat16


def dot(a, b):
    return jnp.dot(a, b, preferred_element_type=F32)


def rope_table():
    half = HEAD // 2
    angle = np.float32(CACHE - 1) * np.float32(THETA) ** (-np.arange(half, dtype=np.float32) / np.float32(half))
    cos, sin = np.cos(angle), np.sin(angle)
    table = np.zeros((8, HEAD), np.float32)
    table[0] = np.concatenate([cos, cos])
    table[1] = np.concatenate([-sin, sin])
    return table


def normed(parts, gain):
    total = parts[0] * parts[0]
    for p in parts[1:]:
        total = total + p * p
    scale = lax.rsqrt(jnp.sum(total, -1, keepdims=True) * (1.0 / D) + 1e-6)
    return [(p * scale * gain[j : j + 1]).astype(BF16) for j, p in enumerate(parts)]


def kernel(
    x_hbm, k_hbm, v_hbm, ga_hbm, wq_hbm, wo_hbm, gm_hbm, wg_hbm, wu_hbm, wd_hbm, rope_hbm, y_hbm,
    xb, ga, gm, rope, wq, wo, wm, kbuf, vbuf, q_s, w_s, o_s, act, hid,
    t1, r1, a1, b1, hb, t2, r2, a2, b2, yb,
    in_sem, k_sem, v_sem, wm_sem, s1, s2, y_sem,
):
    tp = lax.axis_index("tp")
    core = lax.rem(tp, 2)
    chip = tp // 2
    other = 1 - core
    mate = {"tp": chip * 2 + other}
    across = {"tp": (1 - chip) * 2 + core}

    barrier = pltpu.get_barrier_semaphore()
    for device in (mate, across):
        pl.semaphore_signal(barrier, inc=1, device_id=device, device_id_type=MESH)

    def k_copy(i):
        slot = lax.rem(i, DEPTH)
        return pltpu.make_async_copy(k_hbm.at[i // PER, :, lax.rem(i, PER)], kbuf.at[slot], k_sem.at[slot])

    def v_copy(i):
        slot = lax.rem(i, DEPTH)
        return pltpu.make_async_copy(v_hbm.at[i // PER, :, lax.rem(i, PER)], vbuf.at[slot], v_sem.at[slot])

    def wm_copy(w_hbm, n, piece):
        cols = pl.ds(pl.multiple_of(n * NCOL, NCOL), NCOL)
        return pltpu.make_async_copy(w_hbm.at[:, cols], wm.at[piece], wm_sem.at[piece])

    firsts = [
        pltpu.make_async_copy(src, dst, in_sem.at[n])
        for n, (src, dst) in enumerate([(x_hbm, xb), (ga_hbm, ga), (rope_hbm, rope), (wq_hbm, wq), (gm_hbm, gm)])
    ]
    wo_copy = pltpu.make_async_copy(wo_hbm, wo, in_sem.at[5])
    for c in firsts:
        c.start()

    @pl.loop(0, DEPTH)
    def _(i):
        k_copy(i).start()
        v_copy(i).start()

    for c in firsts:
        c.wait()
    blocks = [xb[:, j * 128 : (j + 1) * 128].astype(F32) for j in range(D // 128)]
    for j, b in enumerate(normed(blocks, ga[...].astype(F32))):
        act[:, j * 128 : (j + 1) * 128] = b
    q = dot(act[...], wq[...]).astype(BF16).astype(F32)
    cos, sin = rope[0:1, :], rope[1:2, :]
    for h in range(HEADS):
        t = q[:, h * HEAD : (h + 1) * HEAD]
        t = t * cos + pltpu.roll(t, HEAD // 2, 1) * sin
        q_s[:, h * HEAD : (h + 1) * HEAD] = t.astype(BF16).astype(F32)

    row = lax.broadcasted_iota(jnp.int32, (8, HEAD), 0)

    def scores(i):
        slot = lax.rem(i, DEPTH)
        halves = []
        for s in range(2):
            one = q_s[pl.ds(i // PER * CHUNK + s * PER + lax.rem(i, PER), 1), :]
            lhs = jnp.zeros((8, HEAD), F32)
            for h in range(HEADS):
                lhs = jnp.where(row == 4 * s + h, one[:, h * HEAD : (h + 1) * HEAD], lhs)
            halves.append(lhs)
        lhs = jnp.concatenate(halves, 1).astype(BF16)
        keys = jnp.concatenate([kbuf[slot, 0], kbuf[slot, 1]], 1)
        sc = lax.dot_general(lhs, keys, (((1,), (1,)), ((), ())), preferred_element_type=F32)
        r = lax.broadcasted_iota(jnp.int32, (8, KV), 0)
        c = lax.broadcasted_iota(jnp.int32, (8, KV), 1)
        sc = jnp.where(jnp.bitwise_and(r, 3) == jnp.bitwise_and(c, 3), sc * HEAD**-0.5, -jnp.inf)
        e = jnp.exp(sc - jnp.max(sc, -1, keepdims=True))
        w_s[...] = (e * (1.0 / jnp.sum(e, -1, keepdims=True))).astype(BF16)

    def values(i):
        slot = lax.rem(i, DEPTH)
        vals = jnp.concatenate([vbuf[slot, 0], vbuf[slot, 1]], 1)
        return dot(w_s[...], vals)

    def send(src, dst, sems, n, device):
        return pltpu.make_async_remote_copy(
            src_ref=src, dst_ref=dst, send_sem=sems.at[0, n], recv_sem=sems.at[1, n], device_id=device, device_id_type=MESH
        )

    def first_a(j):
        return send(t1.at[j, other], r1.at[j], s1.at[0], j, mate)

    def first_b(j):
        return send(a1.at[j], b1.at[j], s1.at[1], j, across)

    def first_c(j):
        return send(hb.at[core, j], hb.at[core, j], s1.at[2], j, mate)

    def project(j):
        o = jnp.concatenate(
            [
                jnp.concatenate([o_s[pl.ds(j * PER, PER), 4 * s + h, s * HEAD : (s + 1) * HEAD] for h in range(HEADS)], 1)
                for s in range(2)
            ],
            0,
        ).astype(BF16)
        for s in range(2):
            t1[j, s] = dot(o, wo[:, s * HALF : (s + 1) * HALF]).astype(BF16)
        first_a(j).start()

    def fold(j):
        first_a(j).wait()
        a1[j] = (t1[j, core].astype(F32) + r1[j].astype(F32)).astype(BF16)
        first_b(j).start()

    def finish(j):
        first_b(j).wait()
        mine = xb[pl.ds(pl.multiple_of(j * CHUNK, CHUNK), CHUNK), pl.ds(pl.multiple_of(core * HALF, HALF), HALF)].astype(F32)
        hb[core, j] = (mine + (a1[j].astype(F32) + b1[j].astype(F32))).astype(BF16)
        first_c(j).start()

    k_copy(0).wait()
    scores(0)
    k_copy(DEPTH).start()

    @pl.loop(1, PAIRS)
    def _(i):
        k_copy(i).wait()
        v_copy(i - 1).wait()
        out = values(i - 1)
        scores(i)
        o_s[i - 1] = out

        @pl.when(i + DEPTH < PAIRS)
        def _():
            k_copy(i + DEPTH).start()

        @pl.when(i - 1 + DEPTH < PAIRS)
        def _():
            v_copy(i - 1 + DEPTH).start()

        @pl.when(i == 3)
        def _():
            wo_copy.start()

        n = i - 1 + DEPTH - PAIRS

        @pl.when((n >= 0) & (n < PIECES))
        def _():
            wm_copy(wg_hbm, n, n).start()
            wm_copy(wu_hbm, n, PIECES + n).start()

        @pl.when(n == PIECES)
        def _():
            wm_copy(wd_hbm, 0, 2 * PIECES).start()
            wm_copy(wd_hbm, 1, 2 * PIECES + 1).start()

        j = i // PER - 1
        step = lax.rem(i, PER)

        @pl.when(i == PER)
        def _():
            wo_copy.wait()
            pl.semaphore_wait(barrier, 2)

        @pl.when((i >= PER) & (step == 0))
        def _():
            project(j)

        @pl.when((i >= PER) & (step == 2))
        def _():
            fold(j)

        @pl.when((i >= PER) & (step == 5))
        def _():
            finish(j)

    wm_copy(wd_hbm, 2, 2 * PIECES + 2).start()
    wm_copy(wd_hbm, 3, 2 * PIECES + 3).start()
    v_copy(PAIRS - 1).wait()
    o_s[PAIRS - 1] = values(PAIRS - 1)
    last = CHUNKS - 1
    project(last)
    fold(last)
    finish(last)
    for j in range(CHUNKS):
        first_c(j).wait()

    h = [hb[s].reshape(ROWS, HALF) for s in range(2)]
    blocks = [h[j // 8][:, (j % 8) * 128 : (j % 8 + 1) * 128].astype(F32) for j in range(D // 128)]
    for j, b in enumerate(normed(blocks, gm[...].astype(F32))):
        act[:, j * 128 : (j + 1) * 128] = b

    @pl.loop(0, PIECES)
    def _(n):
        wm_copy(wg_hbm, n, n).wait()
        wm_copy(wu_hbm, n, PIECES + n).wait()
        gate = dot(act[...], wm[n])
        up = dot(act[...], wm[PIECES + n])
        hid[n] = (gate * (1.0 / (1.0 + jnp.exp(-gate))) * up).astype(BF16)

    def second_a(n):
        return send(t2.at[n, other], r2.at[n], s2.at[0], n, mate)

    def second_b(n):
        return send(a2.at[n], b2.at[n], s2.at[1], n, across)

    def cols_of(n):
        return pl.ds(pl.multiple_of(n * NCOL + core * (NCOL // 2), NCOL // 2), NCOL // 2)

    def second_c(n):
        return send(yb.at[n], y_hbm.at[:, cols_of(n)], s2.at[2], n, mate)

    def y_copy(n):
        return pltpu.make_async_copy(yb.at[n], y_hbm.at[:, cols_of(n)], y_sem.at[n])

    @pl.loop(0, PIECES)
    def _(n):
        wm_copy(wd_hbm, n, 2 * PIECES + n).wait()
        t = dot(hid[0], wm[2 * PIECES + n, 0:NCOL])
        for m in range(1, PIECES):
            t = t + dot(hid[m], wm[2 * PIECES + n, m * NCOL : (m + 1) * NCOL])
        for s in range(2):
            t2[n, s] = t[:, s * (NCOL // 2) : (s + 1) * (NCOL // 2)].astype(BF16)
        second_a(n).start()

    @pl.loop(0, PIECES)
    def _(n):
        second_a(n).wait()
        a2[n] = (t2[n, core].astype(F32) + r2[n].astype(F32)).astype(BF16)
        second_b(n).start()

    @pl.loop(0, PIECES)
    def _(n):
        second_b(n).wait()
        off = pl.multiple_of(lax.rem(n, 2) * NCOL + core * (NCOL // 2), NCOL // 2)
        mine = hb[n // 2, :, :, pl.ds(off, NCOL // 2)].reshape(ROWS, NCOL // 2).astype(F32)
        yb[n] = (mine + (a2[n].astype(F32) + b2[n].astype(F32))).astype(BF16)
        second_c(n).start()
        y_copy(n).start()

    @pl.loop(0, PIECES)
    def _(n):
        second_c(n).wait()
        y_copy(n).wait()


def layer(x, k_cache, v_cache, gain_a, wq, wo, gain_m, w_gate, w_up, w_down):
    hbm = pl.BlockSpec(memory_space=pl.ANY)
    vmem, dma = pltpu.VMEM, pltpu.SemaphoreType.DMA
    return pl.pallas_call(
        kernel,
        out_shape=jax.ShapeDtypeStruct((ROWS, D), BF16),
        in_specs=[hbm] * 11,
        out_specs=hbm,
        scratch_shapes=[
            vmem((ROWS, D), BF16),
            vmem((D // 128, 128), BF16),
            vmem((D // 128, 128), BF16),
            vmem((8, HEAD), F32),
            vmem((D, HEADS * HEAD), BF16),
            vmem((HEADS * HEAD, D), BF16),
            vmem((3 * PIECES, D, NCOL), BF16),
            vmem((DEPTH, 2, KV, HEAD), BF16),
            vmem((DEPTH, 2, KV, HEAD), BF16),
            vmem((ROWS, HEADS * HEAD), F32),
            vmem((8, KV), BF16),
            vmem((PAIRS, 8, 2 * HEAD), F32),
            vmem((ROWS, D), BF16),
            vmem((PIECES, ROWS, NCOL), BF16),
            vmem((CHUNKS, 2, CHUNK, HALF), BF16),
            vmem((CHUNKS, CHUNK, HALF), BF16),
            vmem((CHUNKS, CHUNK, HALF), BF16),
            vmem((CHUNKS, CHUNK, HALF), BF16),
            vmem((2, CHUNKS, CHUNK, HALF), BF16),
            vmem((PIECES, 2, ROWS, NCOL // 2), BF16),
            vmem((PIECES, ROWS, NCOL // 2), BF16),
            vmem((PIECES, ROWS, NCOL // 2), BF16),
            vmem((PIECES, ROWS, NCOL // 2), BF16),
            vmem((PIECES, ROWS, NCOL // 2), BF16),
            dma((6,)),
            dma((DEPTH,)),
            dma((DEPTH,)),
            dma((3 * PIECES,)),
            dma((3, 2, CHUNKS)),
            dma((3, 2, PIECES)),
            dma((PIECES,)),
        ],
        compiler_params=pltpu.CompilerParams(collective_id=0, has_side_effects=True, vmem_limit_bytes=67043328),
    )(
        x,
        k_cache.reshape(CHUNKS, 2, PER, KV, HEAD),
        v_cache.reshape(CHUNKS, 2, PER, KV, HEAD),
        gain_a.reshape(D // 128, 128),
        wq,
        wo,
        gain_m.reshape(D // 128, 128),
        w_gate,
        w_up,
        w_down,
        jnp.asarray(rope_table()),
    )


def solution(mesh):
    states, cache, columns, rows_of = P("dp", None), P("dp", None, "tp", None), P(None, "tp"), P("tp", None)
    return jax.shard_map(
        layer,
        mesh=mesh,
        in_specs=(states, cache, cache, P(None), columns, rows_of, P(None), columns, columns, rows_of),
        out_specs=states,
        check_vma=False,
    )
```

```python
import jax
import jax.numpy as jnp
import numpy as np
from jax import lax
from jax.experimental import pallas as pl
from jax.experimental.pallas import tpu as pltpu
from jax.sharding import PartitionSpec as P

MESH = pl.DeviceIdType.MESH
HEAD = 128
THETA = 10000
ROWS, D, CACHE, HEADS = 64, 2048, 1024, 4
KV = CACHE * HEADS
PAIRS = ROWS // 2
DEPTH = 6
CHUNK = 8
CHUNKS = ROWS // CHUNK
PER = CHUNK // 2
HALF = D // 2
FF = 2048
NCOL = 512
PIECES = D // NCOL
F32, BF16 = jnp.float32, jnp.bfloat16


def dot(a, b):
    return jnp.dot(a, b, preferred_element_type=F32)


def rope_table():
    half = HEAD // 2
    angle = np.float32(CACHE - 1) * np.float32(THETA) ** (-np.arange(half, dtype=np.float32) / np.float32(half))
    cos, sin = np.cos(angle), np.sin(angle)
    table = np.zeros((8, HEAD), np.float32)
    table[0] = np.concatenate([cos, cos])
    table[1] = np.concatenate([-sin, sin])
    return table


def normed(parts, gain):
    total = parts[0] * parts[0]
    for p in parts[1:]:
        total = total + p * p
    scale = lax.rsqrt(jnp.sum(total, -1, keepdims=True) * (1.0 / D) + 1e-6)
    return [(p * scale * gain[j : j + 1]).astype(BF16) for j, p in enumerate(parts)]


def kernel(
    x_hbm, k_hbm, v_hbm, ga_hbm, wq_hbm, wo_hbm, gm_hbm, wg_hbm, wu_hbm, wd_hbm, rope_hbm, y,
    xb, ga, gm, rope, wq, wo, wm, kbuf, vbuf, q_s, s_s, o_s, act, hid,
    t1, r1, a1, b1, hb, d1, t2, r2, a2, b2,
    in_sem, k_sem, v_sem, wm_sem, s1, sd, s2,
):
    tp = lax.axis_index("tp")
    core = lax.rem(tp, 2)
    chip = tp // 2
    other = 1 - core
    mate = {"tp": chip * 2 + other}
    across = {"tp": (1 - chip) * 2 + core}
    corner = {"tp": (1 - chip) * 2 + other}

    barrier = pltpu.get_barrier_semaphore()
    for device in (mate, across, corner):
        pl.semaphore_signal(barrier, inc=1, device_id=device, device_id_type=MESH)

    def k_copy(i):
        slot = lax.rem(i, DEPTH)
        return pltpu.make_async_copy(k_hbm.at[i // PER, :, lax.rem(i, PER)], kbuf.at[slot], k_sem.at[slot])

    def v_copy(i):
        slot = lax.rem(i, DEPTH)
        return pltpu.make_async_copy(v_hbm.at[i // PER, :, lax.rem(i, PER)], vbuf.at[slot], v_sem.at[slot])

    def wm_copy(w_hbm, n, piece):
        cols = pl.ds(pl.multiple_of(n * NCOL, NCOL), NCOL)
        return pltpu.make_async_copy(w_hbm.at[:, cols], wm.at[piece], wm_sem.at[piece])

    firsts = [
        pltpu.make_async_copy(src, dst, in_sem.at[n])
        for n, (src, dst) in enumerate([(x_hbm, xb), (ga_hbm, ga), (rope_hbm, rope), (wq_hbm, wq), (gm_hbm, gm)])
    ]
    wo_copy = pltpu.make_async_copy(wo_hbm, wo, in_sem.at[5])
    for c in firsts:
        c.start()

    @pl.loop(0, DEPTH)
    def _(i):
        k_copy(i).start()
        v_copy(i).start()

    for c in firsts:
        c.wait()
    blocks = [xb[:, :, j * 128 : (j + 1) * 128].astype(F32).reshape(ROWS, 128) for j in range(D // 128)]
    for j, b in enumerate(normed(blocks, ga[...].astype(F32))):
        act[:, j * 128 : (j + 1) * 128] = b
    q = dot(act[...], wq[...]).astype(BF16).astype(F32)
    cos, sin = rope[0:1, :], rope[1:2, :]
    for h in range(HEADS):
        t = q[:, h * HEAD : (h + 1) * HEAD]
        t = t * cos + pltpu.roll(t, HEAD // 2, 1) * sin
        q_s[:, h * HEAD : (h + 1) * HEAD] = t.astype(BF16).astype(F32)

    row = lax.broadcasted_iota(jnp.int32, (8, HEAD), 0)

    def scores(i):
        slot = lax.rem(i, DEPTH)
        halves = []
        for s in range(2):
            one = q_s[pl.ds(i // PER * CHUNK + s * PER + lax.rem(i, PER), 1), :]
            lhs = jnp.zeros((8, HEAD), F32)
            for h in range(HEADS):
                lhs = jnp.where(row == 4 * s + h, one[:, h * HEAD : (h + 1) * HEAD], lhs)
            halves.append(lhs)
        lhs = jnp.concatenate(halves, 1).astype(BF16)
        keys = jnp.concatenate([kbuf[slot, 0], kbuf[slot, 1]], 1)
        return lax.dot_general(lhs, keys, (((1,), (1,)), ((), ())), preferred_element_type=F32)

    def weights(sc):
        r = lax.broadcasted_iota(jnp.int32, (8, KV), 0)
        c = lax.broadcasted_iota(jnp.int32, (8, KV), 1)
        sc = jnp.where(jnp.bitwise_and(r, 3) == jnp.bitwise_and(c, 3), sc * HEAD**-0.5, -jnp.inf)
        e = jnp.exp(sc - jnp.max(sc, -1, keepdims=True))
        return (e * (1.0 / jnp.sum(e, -1, keepdims=True))).astype(BF16)

    def values(i, w):
        slot = lax.rem(i, DEPTH)
        vals = jnp.concatenate([vbuf[slot, 0], vbuf[slot, 1]], 1)
        return dot(w, vals)

    def send(src, dst, sems, n, device):
        return pltpu.make_async_remote_copy(
            src_ref=src, dst_ref=dst, send_sem=sems.at[0, n], recv_sem=sems.at[1, n], device_id=device, device_id_type=MESH
        )

    def first_a(j):
        return send(t1.at[j, other], r1.at[j], s1.at[0], j, mate)

    def first_b(j):
        return send(a1.at[j], b1.at[j], s1.at[1], j, across)

    def first_c(j):
        return send(hb.at[core, j], hb.at[core, j], s1.at[2], j, mate)

    def direct(n):
        return send(t1.at[CHUNKS - 1], d1.at[n], sd, n, (mate, across, corner)[n])

    def project(j):
        o = jnp.concatenate(
            [
                jnp.concatenate([o_s[pl.ds(j * PER, PER), 4 * s + h, s * HEAD : (s + 1) * HEAD] for h in range(HEADS)], 1)
                for s in range(2)
            ],
            0,
        ).astype(BF16)
        for s in range(2):
            t1[j, s] = dot(o, wo[:, s * HALF : (s + 1) * HALF]).astype(BF16)

    def fold(j):
        first_a(j).wait()
        a1[j] = (t1[j, core].astype(F32) + r1[j].astype(F32)).astype(BF16)
        first_b(j).start()

    def finish(j):
        first_b(j).wait()
        mine = xb[j, :, pl.ds(pl.multiple_of(core * HALF, HALF), HALF)].astype(F32)
        hb[core, j] = (mine + (a1[j].astype(F32) + b1[j].astype(F32))).astype(BF16)
        first_c(j).start()

    k_copy(0).wait()
    s_s[...] = scores(0)
    k_copy(DEPTH).start()

    @pl.loop(1, PAIRS)
    def _(i):
        k_copy(i).wait()
        v_copy(i - 1).wait()
        w = weights(s_s[...])
        sc = scores(i)
        o_s[i - 1] = values(i - 1, w)
        s_s[...] = sc

        @pl.when(i + DEPTH < PAIRS)
        def _():
            k_copy(i + DEPTH).start()

        @pl.when(i - 1 + DEPTH < PAIRS)
        def _():
            v_copy(i - 1 + DEPTH).start()

        @pl.when(i == 3)
        def _():
            wo_copy.start()

        n = i - 1 + DEPTH - PAIRS

        @pl.when((n >= 0) & (n < PIECES))
        def _():
            wm_copy(wg_hbm, n, n).start()
            wm_copy(wu_hbm, n, PIECES + n).start()

        @pl.when(n == PIECES)
        def _():
            wm_copy(wd_hbm, 0, 2 * PIECES).start()
            wm_copy(wd_hbm, 1, 2 * PIECES + 1).start()

        j = i // PER - 1
        step = lax.rem(i, PER)

        @pl.when(i == PER)
        def _():
            wo_copy.wait()
            pl.semaphore_wait(barrier, 3)

        @pl.when((i >= PER) & (step == 0))
        def _():
            project(j)
            first_a(j).start()

        @pl.when((i >= PER) & (step == 2))
        def _():
            fold(j)

        @pl.when((i >= 2 * PER) & (step == 3))
        def _():
            finish(j - 1)

    wm_copy(wd_hbm, 2, 2 * PIECES + 2).start()
    wm_copy(wd_hbm, 3, 2 * PIECES + 3).start()
    w = weights(s_s[...])
    v_copy(PAIRS - 1).wait()
    o_s[PAIRS - 1] = values(PAIRS - 1, w)
    last = CHUNKS - 1
    project(last)
    for n in range(3):
        direct(n).start()
    finish(last - 1)
    for j in range(last):
        first_c(j).wait()
    for n in range(3):
        direct(n).wait()
    for s in range(2):
        near = t1[last, s].astype(F32) + d1[0, s].astype(F32)
        far = d1[1, s].astype(F32) + d1[2, s].astype(F32)
        hb[s, last] = (xb[last, :, s * HALF : (s + 1) * HALF].astype(F32) + (near + far)).astype(BF16)

    h = [hb[s].astype(F32).reshape(ROWS, HALF) for s in range(2)]
    blocks = [h[j // 8][:, (j % 8) * 128 : (j % 8 + 1) * 128] for j in range(D // 128)]
    for j, b in enumerate(normed(blocks, gm[...].astype(F32))):
        act[:, j * 128 : (j + 1) * 128] = b

    for n in range(PIECES):
        wm_copy(wg_hbm, n, n).wait()
        wm_copy(wu_hbm, n, PIECES + n).wait()
    for n in range(FF // 256):
        cols = slice(n % 2 * 256, n % 2 * 256 + 256)
        gate = dot(act[...], wm[n // 2, :, cols])
        up = dot(act[...], wm[PIECES + n // 2, :, cols])
        hid[:, n * 256 : (n + 1) * 256] = (gate * (1.0 / (1.0 + jnp.exp(-gate))) * up).astype(BF16)

    def second_a(n):
        return send(t2.at[n, other], r2.at[n], s2.at[0], n, mate)

    def second_b(n):
        return send(a2.at[n], b2.at[n], s2.at[1], n, across)

    def cols_of(n):
        return pl.ds(pl.multiple_of(n * NCOL + core * (NCOL // 2), NCOL // 2), NCOL // 2)

    def second_c(n):
        return send(y.at[:, cols_of(n)], y.at[:, cols_of(n)], s2.at[2], n, mate)

    for n in range(PIECES):
        wm_copy(wd_hbm, n, 2 * PIECES + n).wait()
        for s in range(2):
            t2[n, s] = dot(hid[...], wm[2 * PIECES + n, :, s * (NCOL // 2) : (s + 1) * (NCOL // 2)]).astype(BF16)
        second_a(n).start()
    for n in range(PIECES):
        second_a(n).wait()
        a2[n] = (t2[n, core].astype(F32) + r2[n].astype(F32)).astype(BF16)
        second_b(n).start()
    for n in range(PIECES):
        second_b(n).wait()
        off = pl.multiple_of(n % 2 * NCOL + core * (NCOL // 2), NCOL // 2)
        mine = hb[n // 2, :, :, pl.ds(off, NCOL // 2)].astype(F32).reshape(ROWS, NCOL // 2)
        y[:, cols_of(n)] = (mine + (a2[n].astype(F32) + b2[n].astype(F32))).astype(BF16)
        second_c(n).start()
    for n in range(PIECES):
        second_c(n).wait()


def layer(x, k_cache, v_cache, gain_a, wq, wo, gain_m, w_gate, w_up, w_down):
    hbm = pl.BlockSpec(memory_space=pl.ANY)
    vmem, dma = pltpu.VMEM, pltpu.SemaphoreType.DMA
    return pl.pallas_call(
        kernel,
        out_shape=pltpu.VMEM((ROWS, D), BF16),
        in_specs=[hbm] * 11,
        out_specs=pl.BlockSpec(memory_space=pltpu.VMEM),
        scratch_shapes=[
            vmem((CHUNKS, CHUNK, D), BF16),
            vmem((D // 128, 128), BF16),
            vmem((D // 128, 128), BF16),
            vmem((8, HEAD), F32),
            vmem((D, HEADS * HEAD), BF16),
            vmem((HEADS * HEAD, D), BF16),
            vmem((3 * PIECES, D, NCOL), BF16),
            vmem((DEPTH, 2, KV, HEAD), BF16),
            vmem((DEPTH, 2, KV, HEAD), BF16),
            vmem((ROWS, HEADS * HEAD), F32),
            vmem((8, KV), F32),
            vmem((PAIRS, 8, 2 * HEAD), F32),
            vmem((ROWS, D), BF16),
            vmem((ROWS, FF), BF16),
            vmem((CHUNKS, 2, CHUNK, HALF), BF16),
            vmem((CHUNKS, CHUNK, HALF), BF16),
            vmem((CHUNKS, CHUNK, HALF), BF16),
            vmem((CHUNKS, CHUNK, HALF), BF16),
            vmem((2, CHUNKS, CHUNK, HALF), BF16),
            vmem((3, 2, CHUNK, HALF), BF16),
            vmem((PIECES, 2, ROWS, NCOL // 2), BF16),
            vmem((PIECES, ROWS, NCOL // 2), BF16),
            vmem((PIECES, ROWS, NCOL // 2), BF16),
            vmem((PIECES, ROWS, NCOL // 2), BF16),
            dma((6,)),
            dma((DEPTH,)),
            dma((DEPTH,)),
            dma((3 * PIECES,)),
            dma((3, 2, CHUNKS)),
            dma((2, 3)),
            dma((3, 2, PIECES)),
        ],
        compiler_params=pltpu.CompilerParams(collective_id=0, has_side_effects=True, vmem_limit_bytes=62000000),
    )(
        x.reshape(CHUNKS, CHUNK, D),
        k_cache.reshape(CHUNKS, 2, PER, KV, HEAD),
        v_cache.reshape(CHUNKS, 2, PER, KV, HEAD),
        gain_a.reshape(D // 128, 128),
        wq,
        wo,
        gain_m.reshape(D // 128, 128),
        w_gate,
        w_up,
        w_down,
        jnp.asarray(rope_table()),
    )


def solution(mesh):
    states, cache, columns, rows_of = P("dp", None), P("dp", None, "tp", None), P(None, "tp"), P("tp", None)
    return jax.shard_map(
        layer,
        mesh=mesh,
        in_specs=(states, cache, cache, P(None), columns, rows_of, P(None), columns, columns, rows_of),
        out_specs=states,
        check_vma=False,
    )
```

```python
import jax
import jax.numpy as jnp
import numpy as np
from jax import lax
from jax.experimental import pallas as pl
from jax.experimental.pallas import tpu as pltpu
from jax.sharding import PartitionSpec as P

MESH = pl.DeviceIdType.MESH
HEAD = 128
THETA = 10000
ROWS, D, CACHE, HEADS = 64, 2048, 1024, 4
KV = CACHE * HEADS
PAIRS = ROWS // 2
DEPTH = 6
CHUNK = 8
CHUNKS = ROWS // CHUNK
PER = CHUNK // 2
HALF = D // 2
FF = 2048
NCOL = 512
PIECES = D // NCOL
SUB = 256
SUBS = HALF // SUB
F32, BF16 = jnp.float32, jnp.bfloat16


def dot(a, b):
    return jnp.dot(a, b, preferred_element_type=F32)


def rope_table():
    half = HEAD // 2
    angle = np.float32(CACHE - 1) * np.float32(THETA) ** (-np.arange(half, dtype=np.float32) / np.float32(half))
    cos, sin = np.cos(angle), np.sin(angle)
    table = np.zeros((8, HEAD), np.float32)
    table[0] = np.concatenate([cos, cos])
    table[1] = np.concatenate([-sin, sin])
    return table


def normed(parts, gain):
    total = parts[0] * parts[0]
    for p in parts[1:]:
        total = total + p * p
    scale = lax.rsqrt(jnp.sum(total, -1, keepdims=True) * (1.0 / D) + 1e-6)
    return [(p * scale * gain[j : j + 1]).astype(BF16) for j, p in enumerate(parts)]


def kernel(
    x_hbm, k_hbm, v_hbm, ga_hbm, wq_hbm, wo_hbm, gm_hbm, wg_hbm, wu_hbm, wd_hbm, rope_hbm, y,
    xb, ga, gm, rope, wq, wo, wm, kbuf, vbuf, q_s, s_s, o_s, act, hid,
    t1, r1, a1, b1, hb, d1, t2, r2, a2, b2,
    in_sem, k_sem, v_sem, wm_sem, s1, sd, s2,
):
    tp = lax.axis_index("tp")
    core = lax.rem(tp, 2)
    chip = tp // 2
    other = 1 - core
    mate = {"tp": chip * 2 + other}
    across = {"tp": (1 - chip) * 2 + core}
    corner = {"tp": (1 - chip) * 2 + other}

    barrier = pltpu.get_barrier_semaphore()
    for device in (mate, across, corner):
        pl.semaphore_signal(barrier, inc=1, device_id=device, device_id_type=MESH)

    def k_copy(i):
        slot = lax.rem(i, DEPTH)
        return pltpu.make_async_copy(k_hbm.at[i // PER, :, lax.rem(i, PER)], kbuf.at[slot], k_sem.at[slot])

    def v_copy(i):
        slot = lax.rem(i, DEPTH)
        return pltpu.make_async_copy(v_hbm.at[i // PER, :, lax.rem(i, PER)], vbuf.at[slot], v_sem.at[slot])

    def wm_copy(w_hbm, n, piece):
        start = n * NCOL if w_hbm is not wd_hbm else lax.rem(n // 2 + other, 2) * HALF + n % 2 * NCOL
        cols = pl.ds(pl.multiple_of(start, NCOL), NCOL)
        return pltpu.make_async_copy(w_hbm.at[:, cols], wm.at[piece], wm_sem.at[piece])

    firsts = [
        pltpu.make_async_copy(src, dst, in_sem.at[n])
        for n, (src, dst) in enumerate([(x_hbm, xb), (ga_hbm, ga), (rope_hbm, rope), (wq_hbm, wq), (gm_hbm, gm)])
    ]
    wo_copy = pltpu.make_async_copy(wo_hbm, wo, in_sem.at[5])
    for c in firsts:
        c.start()

    @pl.loop(0, DEPTH)
    def _(i):
        k_copy(i).start(priority=1)
        v_copy(i).start(priority=1)

    for c in firsts:
        c.wait()
    blocks = [xb[:, :, j * 128 : (j + 1) * 128].astype(F32).reshape(ROWS, 128) for j in range(D // 128)]
    for j, b in enumerate(normed(blocks, ga[...].astype(F32))):
        act[:, j * 128 : (j + 1) * 128] = b
    q = dot(act[...], wq[...]).astype(BF16).astype(F32)
    cos, sin = rope[0:1, :], rope[1:2, :]
    for h in range(HEADS):
        t = q[:, h * HEAD : (h + 1) * HEAD]
        t = t * cos + pltpu.roll(t, HEAD // 2, 1) * sin
        q_s[:, h * HEAD : (h + 1) * HEAD] = t.astype(BF16).astype(F32)

    row = lax.broadcasted_iota(jnp.int32, (8, HEAD), 0)

    def scores(i):
        slot = lax.rem(i, DEPTH)
        halves = []
        for s in range(2):
            one = q_s[pl.ds(i // PER * CHUNK + s * PER + lax.rem(i, PER), 1), :]
            lhs = jnp.zeros((8, HEAD), F32)
            for h in range(HEADS):
                lhs = jnp.where(row == 4 * s + h, one[:, h * HEAD : (h + 1) * HEAD], lhs)
            halves.append(lhs)
        lhs = jnp.concatenate(halves, 1).astype(BF16)
        keys = jnp.concatenate([kbuf[slot, 0], kbuf[slot, 1]], 1)
        return lax.dot_general(lhs, keys, (((1,), (1,)), ((), ())), preferred_element_type=F32)

    def weights(sc):
        r = lax.broadcasted_iota(jnp.int32, (8, KV), 0)
        c = lax.broadcasted_iota(jnp.int32, (8, KV), 1)
        sc = jnp.where(jnp.bitwise_and(r, 3) == jnp.bitwise_and(c, 3), sc * HEAD**-0.5, -jnp.inf)
        e = jnp.exp(sc - jnp.max(sc, -1, keepdims=True))
        return (e * (1.0 / jnp.sum(e, -1, keepdims=True))).astype(BF16)

    def values(i, w):
        slot = lax.rem(i, DEPTH)
        vals = jnp.concatenate([vbuf[slot, 0], vbuf[slot, 1]], 1)
        return dot(w, vals)

    def send(src, dst, sems, n, device):
        return pltpu.make_async_remote_copy(
            src_ref=src, dst_ref=dst, send_sem=sems.at[0, n], recv_sem=sems.at[1, n], device_id=device, device_id_type=MESH
        )

    def first_a(j):
        return send(t1.at[j, other], r1.at[j], s1.at[0], j, mate)

    def first_b(j):
        return send(a1.at[j], b1.at[j], s1.at[1], j, across)

    def first_c(j):
        return send(hb.at[core, j], hb.at[core, j], s1.at[2], j, mate)

    def direct(n):
        return send(t1.at[CHUNKS - 1], d1.at[n], sd, n, (mate, across, corner)[n])

    def project(j):
        o = jnp.concatenate(
            [
                jnp.concatenate([o_s[pl.ds(j * PER, PER), 4 * s + h, s * HEAD : (s + 1) * HEAD] for h in range(HEADS)], 1)
                for s in range(2)
            ],
            0,
        ).astype(BF16)
        for s in range(2):
            t1[j, s] = dot(o, wo[:, s * HALF : (s + 1) * HALF]).astype(BF16)

    def fold(j):
        first_a(j).wait()
        a1[j] = (t1[j, core].astype(F32) + r1[j].astype(F32)).astype(BF16)
        first_b(j).start()

    def finish(j):
        first_b(j).wait()
        mine = xb[j, :, pl.ds(pl.multiple_of(core * HALF, HALF), HALF)].astype(F32)
        hb[core, j] = (mine + (a1[j].astype(F32) + b1[j].astype(F32))).astype(BF16)
        first_c(j).start()

    k_copy(0).wait()
    s_s[...] = scores(0)
    k_copy(DEPTH).start(priority=1)

    @pl.loop(1, PAIRS - 1)
    def _(i):
        k_copy(i).wait()
        v_copy(i - 1).wait()
        w = weights(s_s[...])
        sc = scores(i)
        o_s[i - 1] = values(i - 1, w)
        s_s[...] = sc

        @pl.when(i + DEPTH < PAIRS)
        def _():
            k_copy(i + DEPTH).start(priority=1)

        @pl.when(i - 1 + DEPTH < PAIRS)
        def _():
            v_copy(i - 1 + DEPTH).start(priority=1)

        @pl.when(i == 3)
        def _():
            wo_copy.start()

        n = i - 1 + DEPTH - PAIRS

        @pl.when((n >= 0) & (n < PIECES))
        def _():
            wm_copy(wg_hbm, n, n).start(priority=1)
            wm_copy(wu_hbm, n, PIECES + n).start(priority=1)

        j = i // PER - 1
        step = lax.rem(i, PER)

        @pl.when(i == PER)
        def _():
            wo_copy.wait()
            pl.semaphore_wait(barrier, 3)

        @pl.when((i >= PER) & (step == 0))
        def _():
            project(j)
            first_a(j).start()

        @pl.when((i >= PER) & (step == 2))
        def _():
            fold(j)

        @pl.when((i >= 2 * PER) & (step == 3))
        def _():
            finish(j - 1)

    wm_copy(wd_hbm, 0, 2 * PIECES).start(priority=1)
    wm_copy(wd_hbm, 1, 2 * PIECES + 1).start(priority=1)
    k_copy(PAIRS - 1).wait()
    w = weights(s_s[...])
    s_s[...] = scores(PAIRS - 1)
    wm_copy(wd_hbm, 2, 2 * PIECES + 2).start(priority=1)
    v_copy(PAIRS - 2).wait()
    o_s[PAIRS - 2] = values(PAIRS - 2, w)
    w = weights(s_s[...])
    wm_copy(wd_hbm, 3, 2 * PIECES + 3).start(priority=1)
    v_copy(PAIRS - 1).wait()
    o_s[PAIRS - 1] = values(PAIRS - 1, w)
    last = CHUNKS - 1
    project(last)
    for n in range(3):
        direct(n).start()

    def normed_rows(rows):
        h = [hb[s, rows].astype(F32).reshape(-1, HALF) for s in range(2)]
        blocks = [h[j // 8][:, (j % 8) * 128 : (j % 8 + 1) * 128] for j in range(D // 128)]
        return jnp.concatenate(normed(blocks, gm[...].astype(F32)), 1)

    finish(last - 2)
    finish(last - 1)
    for j in range(last):
        first_c(j).wait()
    done = normed_rows(slice(0, last))
    act[0 : last * CHUNK] = done
    for n in range(3):
        direct(n).wait()
    for s in range(2):
        near = t1[last, s].astype(F32) + d1[0, s].astype(F32)
        far = d1[1, s].astype(F32) + d1[2, s].astype(F32)
        hb[s, last] = (xb[last, :, s * HALF : (s + 1) * HALF].astype(F32) + (near + far)).astype(BF16)
    act[last * CHUNK :] = normed_rows(slice(last, CHUNKS))

    def hidden(n):
        cols = slice(n % 2 * 256, n % 2 * 256 + 256)
        return dot(act[...], wm[n // 2, :, cols]), dot(act[...], wm[PIECES + n // 2, :, cols])

    def keep(n, gate, up):
        hid[:, n * 256 : (n + 1) * 256] = (gate * (1.0 / (1.0 + jnp.exp(-gate))) * up).astype(BF16)

    late = None
    for n in range(FF // 256):
        for m in {0: range(PIECES - 1), FF // 256 - 2: range(PIECES - 1, PIECES)}.get(n, ()):
            wm_copy(wg_hbm, m, m).wait()
            wm_copy(wu_hbm, m, PIECES + m).wait()
        pair = hidden(n)
        if late is not None:
            keep(n - 1, *late)
        late = pair
    keep(FF // 256 - 1, *late)

    def second_a(u):
        return send(t2.at[u], r2.at[u], s2.at[0], u, mate)

    def second_b(u):
        return send(a2.at[u], b2.at[u], s2.at[1], u, across)

    def cols_of(u):
        return pl.ds(pl.multiple_of(core * HALF + u * SUB, SUB), SUB)

    def second_c(u):
        return send(y.at[:, cols_of(u)], y.at[:, cols_of(u)], s2.at[2], u, mate)

    def down(half, u):
        n = half * 2 + u * SUB // NCOL
        if u * SUB % NCOL == 0:
            wm_copy(wd_hbm, n, 2 * PIECES + n).wait()
        return dot(hid[...], wm[2 * PIECES + n, :, u * SUB % NCOL : u * SUB % NCOL + SUB])

    ahead = down(0, 0)
    for u in range(SUBS):
        t = ahead
        if u + 1 < SUBS:
            ahead = down(0, u + 1)
        t2[u] = t.astype(BF16)
        second_a(u).start()
    for first in range(0, SUBS, 2):
        terms = [down(1, u) for u in range(first, first + 2)]
        for u, t in enumerate(terms, first):
            second_a(u).wait()
            a2[u] = (t + r2[u].astype(F32)).astype(BF16)
            second_b(u).start()
    for u in range(SUBS):
        second_b(u).wait()
        mine = hb[core, :, :, u * SUB : (u + 1) * SUB].astype(F32).reshape(ROWS, SUB)
        y[:, cols_of(u)] = (mine + (a2[u].astype(F32) + b2[u].astype(F32))).astype(BF16)
        second_c(u).start()
    for u in range(SUBS):
        second_c(u).wait()


def layer(x, k_cache, v_cache, gain_a, wq, wo, gain_m, w_gate, w_up, w_down):
    hbm = pl.BlockSpec(memory_space=pl.ANY)
    vmem, dma = pltpu.VMEM, pltpu.SemaphoreType.DMA
    return pl.pallas_call(
        kernel,
        out_shape=pltpu.VMEM((ROWS, D), BF16),
        in_specs=[hbm] * 11,
        out_specs=pl.BlockSpec(memory_space=pltpu.VMEM),
        scratch_shapes=[
            vmem((CHUNKS, CHUNK, D), BF16),
            vmem((D // 128, 128), BF16),
            vmem((D // 128, 128), BF16),
            vmem((8, HEAD), F32),
            vmem((D, HEADS * HEAD), BF16),
            vmem((HEADS * HEAD, D), BF16),
            vmem((3 * PIECES, D, NCOL), BF16),
            vmem((DEPTH, 2, KV, HEAD), BF16),
            vmem((DEPTH, 2, KV, HEAD), BF16),
            vmem((ROWS, HEADS * HEAD), F32),
            vmem((8, KV), F32),
            vmem((PAIRS, 8, 2 * HEAD), F32),
            vmem((ROWS, D), BF16),
            vmem((ROWS, FF), BF16),
            vmem((CHUNKS, 2, CHUNK, HALF), BF16),
            vmem((CHUNKS, CHUNK, HALF), BF16),
            vmem((CHUNKS, CHUNK, HALF), BF16),
            vmem((CHUNKS, CHUNK, HALF), BF16),
            vmem((2, CHUNKS, CHUNK, HALF), BF16),
            vmem((3, 2, CHUNK, HALF), BF16),
            vmem((SUBS, ROWS, SUB), BF16),
            vmem((SUBS, ROWS, SUB), BF16),
            vmem((SUBS, ROWS, SUB), BF16),
            vmem((SUBS, ROWS, SUB), BF16),
            dma((6,)),
            dma((DEPTH,)),
            dma((DEPTH,)),
            dma((3 * PIECES,)),
            dma((3, 2, CHUNKS)),
            dma((2, 3)),
            dma((3, 2, SUBS)),
        ],
        compiler_params=pltpu.CompilerParams(collective_id=0, has_side_effects=True, vmem_limit_bytes=62000000),
    )(
        x.reshape(CHUNKS, CHUNK, D),
        k_cache.reshape(CHUNKS, 2, PER, KV, HEAD),
        v_cache.reshape(CHUNKS, 2, PER, KV, HEAD),
        gain_a.reshape(D // 128, 128),
        wq,
        wo,
        gain_m.reshape(D // 128, 128),
        w_gate,
        w_up,
        w_down,
        jnp.asarray(rope_table()),
    )


def solution(mesh):
    states, cache, columns, rows_of = P("dp", None), P("dp", None, "tp", None), P(None, "tp"), P("tp", None)
    return jax.shard_map(
        layer,
        mesh=mesh,
        in_specs=(states, cache, cache, P(None), columns, rows_of, P(None), columns, columns, rows_of),
        out_specs=states,
        check_vma=False,
    )
```

```python
import jax
import jax.numpy as jnp
import numpy as np
from jax import lax
from jax.experimental import pallas as pl
from jax.experimental.pallas import tpu as pltpu
from jax.sharding import PartitionSpec as P

MESH = pl.DeviceIdType.MESH
HEAD = 128
THETA = 10000
ROWS, D, CACHE, HEADS = 64, 2048, 1024, 4
KV = CACHE * HEADS
PAIRS = ROWS // 2
DEPTH = 6
CHUNK = 8
CHUNKS = ROWS // CHUNK
PER = CHUNK // 2
HALF = D // 2
FF = 2048
TALL = 128
NCOL = 512
PIECES = D // NCOL
SUB = NCOL // 2
F32, BF16 = jnp.float32, jnp.bfloat16


def dot(a, b):
    return jnp.dot(a, b, preferred_element_type=F32)


def rope_table():
    half = HEAD // 2
    angle = np.float32(CACHE - 1) * np.float32(THETA) ** (-np.arange(half, dtype=np.float32) / np.float32(half))
    cos, sin = np.cos(angle), np.sin(angle)
    table = np.zeros((8, HEAD), np.float32)
    table[0] = np.concatenate([cos, cos])
    table[1] = np.concatenate([-sin, sin])
    return table


def normed(parts, gain):
    total = parts[0] * parts[0]
    for p in parts[1:]:
        total = total + p * p
    scale = lax.rsqrt(jnp.sum(total, -1, keepdims=True) * (1.0 / D) + 1e-6)
    return [(p * scale * gain[j : j + 1]).astype(BF16) for j, p in enumerate(parts)]


def kernel(
    x_hbm, k_hbm, v_hbm, ga_hbm, wq_hbm, wo_hbm, gm_hbm, wg_hbm, wu_hbm, wd_hbm, rope_hbm, y,
    xb, ga, gm, rope, wq, wo, wm, kbuf, vbuf, q_s, s_s, o_s, act, hid,
    t1, r1, a1, b1, hb, d1, t2, t3, r2, a2, b2,
    in_sem, k_sem, v_sem, wm_sem, s1, sd, s2,
):
    tp = lax.axis_index("tp")
    core = lax.rem(tp, 2)
    chip = tp // 2
    other = 1 - core
    mate = {"tp": chip * 2 + other}
    corner = {"tp": (1 - chip) * 2 + other}
    far = [{"tp": (1 - chip) * 2 + c} for c in range(2)]
    own = lax.rem(core + chip, 2)
    theirs = 1 - own

    barrier = pltpu.get_barrier_semaphore()
    for device in (mate, *far):
        pl.semaphore_signal(barrier, inc=1, device_id=device, device_id_type=MESH)

    def k_copy(i):
        slot = lax.rem(i, DEPTH)
        return pltpu.make_async_copy(k_hbm.at[i // PER, :, lax.rem(i, PER)], kbuf.at[slot], k_sem.at[slot])

    def v_copy(i):
        slot = lax.rem(i, DEPTH)
        return pltpu.make_async_copy(v_hbm.at[i // PER, :, lax.rem(i, PER)], vbuf.at[slot], v_sem.at[slot])

    def wm_copy(w_hbm, n, piece):
        cols = pl.ds(pl.multiple_of(n * NCOL, NCOL), NCOL)
        return pltpu.make_async_copy(w_hbm.at[:, cols], wm.at[piece], wm_sem.at[piece])

    firsts = [
        pltpu.make_async_copy(src, dst, in_sem.at[n])
        for n, (src, dst) in enumerate([(x_hbm, xb), (ga_hbm, ga), (rope_hbm, rope), (wq_hbm, wq), (gm_hbm, gm)])
    ]
    wo_copy = pltpu.make_async_copy(wo_hbm, wo, in_sem.at[5])
    for c in firsts:
        c.start()

    @pl.loop(0, DEPTH)
    def _(i):
        k_copy(i).start(priority=1)
        v_copy(i).start(priority=1)

    for c in firsts:
        c.wait()
    blocks = [xb[:, :, j * 128 : (j + 1) * 128].astype(F32).reshape(ROWS, 128) for j in range(D // 128)]
    for j, b in enumerate(normed(blocks, ga[...].astype(F32))):
        act[0:ROWS, j * 128 : (j + 1) * 128] = b
    act[ROWS:] = jnp.zeros((TALL - ROWS, D), BF16)
    hid[ROWS:] = jnp.zeros((TALL - ROWS, FF), BF16)
    q = dot(act[0:ROWS], wq[...]).astype(BF16).astype(F32)
    cos, sin = rope[0:1, :], rope[1:2, :]
    for h in range(HEADS):
        t = q[:, h * HEAD : (h + 1) * HEAD]
        t = t * cos + pltpu.roll(t, HEAD // 2, 1) * sin
        q_s[:, h * HEAD : (h + 1) * HEAD] = t.astype(BF16).astype(F32)

    row = lax.broadcasted_iota(jnp.int32, (8, HEAD), 0)

    def scores(i):
        slot = lax.rem(i, DEPTH)
        halves = []
        for s in range(2):
            one = q_s[pl.ds(i // PER * CHUNK + s * PER + lax.rem(i, PER), 1), :]
            lhs = jnp.zeros((8, HEAD), F32)
            for h in range(HEADS):
                lhs = jnp.where(row == 4 * s + h, one[:, h * HEAD : (h + 1) * HEAD], lhs)
            halves.append(lhs)
        lhs = jnp.concatenate(halves, 1).astype(BF16)
        keys = jnp.concatenate([kbuf[slot, 0], kbuf[slot, 1]], 1)
        return lax.dot_general(lhs, keys, (((1,), (1,)), ((), ())), preferred_element_type=F32)

    def weights(sc):
        r = lax.broadcasted_iota(jnp.int32, (8, KV), 0)
        c = lax.broadcasted_iota(jnp.int32, (8, KV), 1)
        sc = jnp.where(jnp.bitwise_and(r, 3) == jnp.bitwise_and(c, 3), sc * HEAD**-0.5, -jnp.inf)
        e = jnp.exp(sc - jnp.max(sc, -1, keepdims=True))
        return (e * (1.0 / jnp.sum(e, -1, keepdims=True))).astype(BF16)

    def values(i, w):
        slot = lax.rem(i, DEPTH)
        vals = jnp.concatenate([vbuf[slot, 0], vbuf[slot, 1]], 1)
        return dot(w, vals)

    def send(src, dst, sems, n, device):
        return pltpu.make_async_remote_copy(
            src_ref=src, dst_ref=dst, send_sem=sems.at[0, n], recv_sem=sems.at[1, n], device_id=device, device_id_type=MESH
        )

    def first_a(j):
        return send(t1.at[j, theirs], r1.at[j], s1.at[0], j, mate)

    def first_b(j):
        return send(a1.at[j], b1.at[j], s1.at[1], j, corner)

    def first_c(j):
        return send(hb.at[own, j], hb.at[own, j], s1.at[2], j, mate)

    def direct(n):
        return pltpu.make_async_remote_copy(
            src_ref=t1.at[CHUNKS - 1],
            dst_ref=d1.at[core if n < 2 else 2],
            send_sem=sd.at[0, n],
            recv_sem=sd.at[1, core if n < 2 else 2],
            device_id=(*far, mate)[n],
            device_id_type=MESH,
        )

    def direct_done():
        for n in range(3):
            direct(n).wait_send()
            pltpu.make_async_remote_copy(
                src_ref=t1.at[CHUNKS - 1], dst_ref=d1.at[n], send_sem=sd.at[0, n], recv_sem=sd.at[1, n], device_id=mate, device_id_type=MESH
            ).wait_recv()

    def project(j):
        o = jnp.concatenate(
            [
                jnp.concatenate([o_s[pl.ds(j * PER, PER), 4 * s + h, s * HEAD : (s + 1) * HEAD] for h in range(HEADS)], 1)
                for s in range(2)
            ],
            0,
        ).astype(BF16)
        for s in range(2):
            t1[j, s] = dot(o, wo[:, s * HALF : (s + 1) * HALF]).astype(BF16)

    def fold(j):
        first_a(j).wait()
        a1[j] = (t1[j, own].astype(F32) + r1[j].astype(F32)).astype(BF16)
        first_b(j).start()

    def finish(j):
        first_b(j).wait()
        mine = xb[j, :, pl.ds(pl.multiple_of(own * HALF, HALF), HALF)].astype(F32)
        hb[own, j] = (mine + (a1[j].astype(F32) + b1[j].astype(F32))).astype(BF16)
        first_c(j).start()

    k_copy(0).wait()
    s_s[...] = scores(0)
    k_copy(DEPTH).start(priority=1)

    @pl.loop(1, PAIRS - 1)
    def _(i):
        k_copy(i).wait()
        v_copy(i - 1).wait()
        w = weights(s_s[...])
        sc = scores(i)
        o_s[i - 1] = values(i - 1, w)
        s_s[...] = sc

        @pl.when(i + DEPTH < PAIRS)
        def _():
            k_copy(i + DEPTH).start(priority=1)

        @pl.when(i - 1 + DEPTH < PAIRS)
        def _():
            v_copy(i - 1 + DEPTH).start(priority=1)

        @pl.when(i == 3)
        def _():
            wo_copy.start()

        n = i - 1 + DEPTH - PAIRS

        @pl.when((n >= 0) & (n < PIECES))
        def _():
            wm_copy(wg_hbm, n, n).start(priority=1)
            wm_copy(wu_hbm, n, PIECES + n).start(priority=1)

        j = i // PER - 1
        step = lax.rem(i, PER)

        @pl.when(i == PER)
        def _():
            wo_copy.wait()
            pl.semaphore_wait(barrier, 3)

        @pl.when((i >= PER) & (step == 0))
        def _():
            project(j)
            first_a(j).start()

        @pl.when((i >= PER) & (step == 2))
        def _():
            fold(j)

        @pl.when((i >= 2 * PER) & (step == 3))
        def _():
            finish(j - 1)

    wm_copy(wd_hbm, 0, 2 * PIECES).start(priority=1)
    wm_copy(wd_hbm, 1, 2 * PIECES + 1).start(priority=1)
    k_copy(PAIRS - 1).wait()
    w = weights(s_s[...])
    s_s[...] = scores(PAIRS - 1)
    wm_copy(wd_hbm, 2, 2 * PIECES + 2).start(priority=1)
    v_copy(PAIRS - 2).wait()
    o_s[PAIRS - 2] = values(PAIRS - 2, w)
    w = weights(s_s[...])
    wm_copy(wd_hbm, 3, 2 * PIECES + 3).start(priority=1)
    v_copy(PAIRS - 1).wait()
    o_s[PAIRS - 1] = values(PAIRS - 1, w)
    last = CHUNKS - 1
    project(last)
    for n in range(3):
        direct(n).start()

    def normed_rows(rows):
        h = [hb[s, rows].astype(F32).reshape(-1, HALF) for s in range(2)]
        blocks = [h[j // 8][:, (j % 8) * 128 : (j % 8 + 1) * 128] for j in range(D // 128)]
        return jnp.concatenate(normed(blocks, gm[...].astype(F32)), 1)

    finish(last - 2)
    finish(last - 1)
    for j in range(last):
        first_c(j).wait()
    done = normed_rows(slice(0, last))
    act[0 : last * CHUNK] = done
    direct_done()
    for s in range(2):
        here = t1[last, s].astype(F32) + d1[2, s].astype(F32)
        there = d1[0, s].astype(F32) + d1[1, s].astype(F32)
        hb[s, last] = (xb[last, :, s * HALF : (s + 1) * HALF].astype(F32) + (here + there)).astype(BF16)
    act[last * CHUNK : ROWS] = normed_rows(slice(last, CHUNKS))

    def hidden(n):
        cols = slice(n % 2 * 256, n % 2 * 256 + 256)
        return dot(act[...], wm[n // 2, :, cols])[:ROWS], dot(act[...], wm[PIECES + n // 2, :, cols])[:ROWS]

    def keep(n, gate, up):
        hid[0:ROWS, n * 256 : (n + 1) * 256] = (gate * (1.0 / (1.0 + jnp.exp(-gate))) * up).astype(BF16)

    late = None
    for n in range(FF // 256):
        for m in {0: (0, 1), 4: (2,), 6: (3,)}.get(n, ()):
            wm_copy(wg_hbm, m, m).wait()
            wm_copy(wu_hbm, m, PIECES + m).wait()
        pair = hidden(n)
        if late is not None:
            keep(n - 1, *late)
        late = pair
    keep(FF // 256 - 1, *late)

    def second_a(n):
        return send(t2.at[n], r2.at[n], s2.at[0], n, mate)

    def second_b(n):
        return send(a2.at[n], b2.at[n], s2.at[1], n, corner)

    def cols_of(n):
        return pl.ds(pl.multiple_of(n * NCOL + own * SUB, SUB), SUB)

    def second_c(n):
        return send(y.at[:, cols_of(n)], y.at[:, cols_of(n)], s2.at[2], n, mate)

    def down(n):
        wm_copy(wd_hbm, n, 2 * PIECES + n).wait()
        t2[n] = dot(hid[...], wm[2 * PIECES + n, :, pl.ds(pl.multiple_of(theirs * SUB, SUB), SUB)])[:ROWS].astype(BF16)
        t3[n] = dot(hid[...], wm[2 * PIECES + n, :, pl.ds(pl.multiple_of(own * SUB, SUB), SUB)])[:ROWS]
        second_a(n).start()

    def cross(n):
        second_a(n).wait()
        a2[n] = (t3[n] + r2[n].astype(F32)).astype(BF16)
        second_b(n).start()

    for n in range(PIECES):
        down(n)
        if n >= 1:
            cross(n - 1)
    cross(PIECES - 1)
    for n in range(PIECES):
        second_b(n).wait()
        off = pl.multiple_of(n % 2 * NCOL + own * SUB, SUB)
        mine = hb[n // 2, :, :, pl.ds(off, SUB)].astype(F32).reshape(ROWS, SUB)
        y[:, cols_of(n)] = (mine + (a2[n].astype(F32) + b2[n].astype(F32))).astype(BF16)
        second_c(n).start()
    for n in range(PIECES):
        second_c(n).wait()


def layer(x, k_cache, v_cache, gain_a, wq, wo, gain_m, w_gate, w_up, w_down):
    hbm = pl.BlockSpec(memory_space=pl.ANY)
    vmem, dma = pltpu.VMEM, pltpu.SemaphoreType.DMA
    return pl.pallas_call(
        kernel,
        out_shape=pltpu.VMEM((ROWS, D), BF16),
        in_specs=[hbm] * 11,
        out_specs=pl.BlockSpec(memory_space=pltpu.VMEM),
        scratch_shapes=[
            vmem((CHUNKS, CHUNK, D), BF16),
            vmem((D // 128, 128), BF16),
            vmem((D // 128, 128), BF16),
            vmem((8, HEAD), F32),
            vmem((D, HEADS * HEAD), BF16),
            vmem((HEADS * HEAD, D), BF16),
            vmem((3 * PIECES, D, NCOL), BF16),
            vmem((DEPTH, 2, KV, HEAD), BF16),
            vmem((DEPTH, 2, KV, HEAD), BF16),
            vmem((ROWS, HEADS * HEAD), F32),
            vmem((8, KV), F32),
            vmem((PAIRS, 8, 2 * HEAD), F32),
            vmem((TALL, D), BF16),
            vmem((TALL, FF), BF16),
            vmem((CHUNKS, 2, CHUNK, HALF), BF16),
            vmem((CHUNKS, CHUNK, HALF), BF16),
            vmem((CHUNKS, CHUNK, HALF), BF16),
            vmem((CHUNKS, CHUNK, HALF), BF16),
            vmem((2, CHUNKS, CHUNK, HALF), BF16),
            vmem((3, 2, CHUNK, HALF), BF16),
            vmem((PIECES, ROWS, SUB), BF16),
            vmem((PIECES, ROWS, SUB), F32),
            vmem((PIECES, ROWS, SUB), BF16),
            vmem((PIECES, ROWS, SUB), BF16),
            vmem((PIECES, ROWS, SUB), BF16),
            dma((6,)),
            dma((DEPTH,)),
            dma((DEPTH,)),
            dma((3 * PIECES,)),
            dma((3, 2, CHUNKS)),
            dma((2, 3)),
            dma((3, 2, PIECES)),
        ],
        compiler_params=pltpu.CompilerParams(collective_id=0, has_side_effects=True, vmem_limit_bytes=62000000),
    )(
        x.reshape(CHUNKS, CHUNK, D),
        k_cache.reshape(CHUNKS, 2, PER, KV, HEAD),
        v_cache.reshape(CHUNKS, 2, PER, KV, HEAD),
        gain_a.reshape(D // 128, 128),
        wq,
        wo,
        gain_m.reshape(D // 128, 128),
        w_gate,
        w_up,
        w_down,
        jnp.asarray(rope_table()),
    )


def solution(mesh):
    states, cache, columns, rows_of = P("dp", None), P("dp", None, "tp", None), P(None, "tp"), P("tp", None)
    return jax.shard_map(
        layer,
        mesh=mesh,
        in_specs=(states, cache, cache, P(None), columns, rows_of, P(None), columns, columns, rows_of),
        out_specs=states,
        check_vma=False,
    )
```

```python
import jax
import jax.numpy as jnp
import numpy as np
from jax import lax
from jax.experimental import pallas as pl
from jax.experimental.pallas import tpu as pltpu
from jax.sharding import PartitionSpec as P

MESH = pl.DeviceIdType.MESH
HEAD = 128
THETA = 10000
ROWS, D, CACHE, HEADS = 64, 2048, 1024, 4
KV = CACHE * HEADS
PAIRS = ROWS // 2
DEPTH = 6
CHUNK = 8
CHUNKS = ROWS // CHUNK
PER = CHUNK // 2
HALF = D // 2
FF = 2048
TALL = 128
NCOL = 512
PIECES = D // NCOL
SUB = NCOL // 2
F32, BF16 = jnp.float32, jnp.bfloat16


def dot(a, b):
    return jnp.dot(a, b, preferred_element_type=F32)


def rope_table():
    half = HEAD // 2
    angle = np.float32(CACHE - 1) * np.float32(THETA) ** (-np.arange(half, dtype=np.float32) / np.float32(half))
    cos, sin = np.cos(angle), np.sin(angle)
    table = np.zeros((8, HEAD), np.float32)
    table[0] = np.concatenate([cos, cos])
    table[1] = np.concatenate([-sin, sin])
    return table


def normed(parts, gain):
    total = parts[0] * parts[0]
    for p in parts[1:]:
        total = total + p * p
    scale = lax.rsqrt(jnp.sum(total, -1, keepdims=True) * (1.0 / D) + 1e-6)
    return [(p * scale * gain[j : j + 1]).astype(BF16) for j, p in enumerate(parts)]


def kernel(
    x_hbm, k_hbm, v_hbm, ga_hbm, wq_hbm, wo_hbm, gm_hbm, wg_hbm, wu_hbm, wd_hbm, rope_hbm, y,
    xb, ga, gm, rope, wq, wo, wm, kbuf, vbuf, q_s, s_s, o_s, act, hid,
    t1, hb, d1, actf, t2, t3, r2, a2, b2,
    in_sem, k_sem, v_sem, wm_sem, sd, s2,
):
    tp = lax.axis_index("tp")
    core = lax.rem(tp, 2)
    chip = tp // 2
    other = 1 - core
    mate = {"tp": chip * 2 + other}
    corner = {"tp": (1 - chip) * 2 + other}
    far = [{"tp": (1 - chip) * 2 + c} for c in range(2)]
    own = lax.rem(core + chip, 2)
    theirs = 1 - own

    barrier = pltpu.get_barrier_semaphore()
    for device in (mate, *far):
        pl.semaphore_signal(barrier, inc=1, device_id=device, device_id_type=MESH)

    def k_copy(i):
        slot = lax.rem(i, DEPTH)
        return pltpu.make_async_copy(k_hbm.at[i // PER, :, lax.rem(i, PER)], kbuf.at[slot], k_sem.at[slot])

    def v_copy(i):
        slot = lax.rem(i, DEPTH)
        return pltpu.make_async_copy(v_hbm.at[i // PER, :, lax.rem(i, PER)], vbuf.at[slot], v_sem.at[slot])

    def wm_copy(w_hbm, n, piece):
        cols = pl.ds(pl.multiple_of(n * NCOL, NCOL), NCOL)
        return pltpu.make_async_copy(w_hbm.at[:, cols], wm.at[piece], wm_sem.at[piece])

    firsts = [
        pltpu.make_async_copy(src, dst, in_sem.at[n])
        for n, (src, dst) in enumerate([(x_hbm, xb), (ga_hbm, ga), (rope_hbm, rope), (wq_hbm, wq), (gm_hbm, gm)])
    ]
    wo_copy = pltpu.make_async_copy(wo_hbm, wo, in_sem.at[5])
    for c in firsts:
        c.start()

    @pl.loop(0, DEPTH)
    def _(i):
        k_copy(i).start(priority=1)
        v_copy(i).start(priority=1)

    for c in firsts:
        c.wait()
    blocks = [xb[:, :, j * 128 : (j + 1) * 128].astype(F32).reshape(ROWS, 128) for j in range(D // 128)]
    for j, b in enumerate(normed(blocks, ga[...].astype(F32))):
        act[0:ROWS, j * 128 : (j + 1) * 128] = b
    act[ROWS:] = jnp.zeros((TALL - ROWS, D), BF16)
    hid[ROWS:] = jnp.zeros((TALL - ROWS, FF), BF16)
    q = dot(act[0:ROWS], wq[...]).astype(BF16).astype(F32)
    cos, sin = rope[0:1, :], rope[1:2, :]
    for h in range(HEADS):
        t = q[:, h * HEAD : (h + 1) * HEAD]
        t = t * cos + pltpu.roll(t, HEAD // 2, 1) * sin
        q_s[:, h * HEAD : (h + 1) * HEAD] = t.astype(BF16).astype(F32)

    row = lax.broadcasted_iota(jnp.int32, (8, HEAD), 0)

    def scores(i):
        slot = lax.rem(i, DEPTH)
        halves = []
        for s in range(2):
            one = q_s[pl.ds(i // PER * CHUNK + s * PER + lax.rem(i, PER), 1), :]
            lhs = jnp.zeros((8, HEAD), F32)
            for h in range(HEADS):
                lhs = jnp.where(row == 4 * s + h, one[:, h * HEAD : (h + 1) * HEAD], lhs)
            halves.append(lhs)
        lhs = jnp.concatenate(halves, 1).astype(BF16)
        keys = jnp.concatenate([kbuf[slot, 0], kbuf[slot, 1]], 1)
        return lax.dot_general(lhs, keys, (((1,), (1,)), ((), ())), preferred_element_type=F32)

    def weights(sc):
        r = lax.broadcasted_iota(jnp.int32, (8, KV), 0)
        c = lax.broadcasted_iota(jnp.int32, (8, KV), 1)
        sc = jnp.where(jnp.bitwise_and(r, 3) == jnp.bitwise_and(c, 3), sc * HEAD**-0.5, -jnp.inf)
        e = jnp.exp(sc - jnp.max(sc, -1, keepdims=True))
        return (e * (1.0 / jnp.sum(e, -1, keepdims=True))).astype(BF16)

    def values(i, w):
        slot = lax.rem(i, DEPTH)
        vals = jnp.concatenate([vbuf[slot, 0], vbuf[slot, 1]], 1)
        return dot(w, vals)

    def send(src, dst, sems, n, device):
        return pltpu.make_async_remote_copy(
            src_ref=src, dst_ref=dst, send_sem=sems.at[0, n], recv_sem=sems.at[1, n], device_id=device, device_id_type=MESH
        )

    def direct(j, n):
        slot = core if n < 2 else 2
        return pltpu.make_async_remote_copy(
            src_ref=t1.at[j],
            dst_ref=d1.at[j, slot],
            send_sem=sd.at[0, n, j],
            recv_sem=sd.at[1, slot, j],
            device_id=(*far, mate)[n],
            device_id_type=MESH,
        )

    def landed(j, n):
        return pltpu.make_async_remote_copy(
            src_ref=t1.at[j], dst_ref=d1.at[j, n], send_sem=sd.at[0, n, j], recv_sem=sd.at[1, n, j], device_id=mate, device_id_type=MESH
        )

    def take(j):
        for n in range(3):
            landed(j, n).wait()
        parts = []
        for s in range(2):
            here = t1[j, s].astype(F32) + d1[j, 2, s].astype(F32)
            there = d1[j, 0, s].astype(F32) + d1[j, 1, s].astype(F32)
            h = (xb[j, :, s * HALF : (s + 1) * HALF].astype(F32) + (here + there)).astype(BF16)
            hb[s, j] = h
            h = h.astype(F32)
            parts += [h[:, k * 128 : (k + 1) * 128] for k in range(HALF // 128)]
        for k, b in enumerate(normed(parts, gm[...].astype(F32))):
            actf[j, :, k * 128 : (k + 1) * 128] = b.astype(F32)

    def project(j):
        o = jnp.concatenate(
            [
                jnp.concatenate([o_s[pl.ds(j * PER, PER), 4 * s + h, s * HEAD : (s + 1) * HEAD] for h in range(HEADS)], 1)
                for s in range(2)
            ],
            0,
        ).astype(BF16)
        for s in range(2):
            t1[j, s] = dot(o, wo[:, s * HALF : (s + 1) * HALF]).astype(BF16)

    k_copy(0).wait()
    s_s[...] = scores(0)
    k_copy(DEPTH).start(priority=1)

    @pl.loop(1, PAIRS - 1)
    def _(i):
        k_copy(i).wait()
        v_copy(i - 1).wait()
        w = weights(s_s[...])
        sc = scores(i)
        o_s[i - 1] = values(i - 1, w)
        s_s[...] = sc

        @pl.when(i + DEPTH < PAIRS)
        def _():
            k_copy(i + DEPTH).start(priority=1)

        @pl.when(i - 1 + DEPTH < PAIRS)
        def _():
            v_copy(i - 1 + DEPTH).start(priority=1)

        @pl.when(i == 3)
        def _():
            wo_copy.start()

        n = i - 1 + DEPTH - PAIRS

        @pl.when((n >= 0) & (n < PIECES))
        def _():
            wm_copy(wg_hbm, n, n).start(priority=1)
            wm_copy(wu_hbm, n, PIECES + n).start(priority=1)

        j = i // PER - 1
        step = lax.rem(i, PER)

        @pl.when(i == PER)
        def _():
            wo_copy.wait()
            pl.semaphore_wait(barrier, 3)

        @pl.when((i >= PER) & (step == 0))
        def _():
            project(j)
            for n in range(3):
                direct(j, n).start()

        @pl.when((i >= 2 * PER) & (step == 3))
        def _():
            take(j - 1)

    wm_copy(wd_hbm, 0, 2 * PIECES).start(priority=1)
    wm_copy(wd_hbm, 1, 2 * PIECES + 1).start(priority=1)
    k_copy(PAIRS - 1).wait()
    w = weights(s_s[...])
    s_s[...] = scores(PAIRS - 1)
    wm_copy(wd_hbm, 2, 2 * PIECES + 2).start(priority=1)
    v_copy(PAIRS - 2).wait()
    o_s[PAIRS - 2] = values(PAIRS - 2, w)
    w = weights(s_s[...])
    wm_copy(wd_hbm, 3, 2 * PIECES + 3).start(priority=1)
    v_copy(PAIRS - 1).wait()
    o_s[PAIRS - 1] = values(PAIRS - 1, w)
    last = CHUNKS - 1
    project(last)
    for n in range(3):
        direct(last, n).start()
    take(last - 2)
    take(last - 1)
    take(last)
    act[0:ROWS] = actf[...].reshape(ROWS, D).astype(BF16)

    def hidden(n):
        cols = slice(n % 2 * 256, n % 2 * 256 + 256)
        return dot(act[...], wm[n // 2, :, cols])[:ROWS], dot(act[...], wm[PIECES + n // 2, :, cols])[:ROWS]

    def keep(n, gate, up):
        hid[0:ROWS, n * 256 : (n + 1) * 256] = (gate * (1.0 / (1.0 + jnp.exp(-gate))) * up).astype(BF16)

    late = None
    for n in range(FF // 256):
        for m in {0: (0, 1), 4: (2,), 6: (3,)}.get(n, ()):
            wm_copy(wg_hbm, m, m).wait()
            wm_copy(wu_hbm, m, PIECES + m).wait()
        pair = hidden(n)
        if late is not None:
            keep(n - 1, *late)
        late = pair
    keep(FF // 256 - 1, *late)

    def second_a(n):
        return send(t2.at[n], r2.at[n], s2.at[0], n, mate)

    def second_b(n):
        return send(a2.at[n], b2.at[n], s2.at[1], n, corner)

    def cols_of(n):
        return pl.ds(pl.multiple_of(n * NCOL + own * SUB, SUB), SUB)

    def second_c(n):
        return send(y.at[:, cols_of(n)], y.at[:, cols_of(n)], s2.at[2], n, mate)

    def down(n):
        wm_copy(wd_hbm, n, 2 * PIECES + n).wait()
        t2[n] = dot(hid[...], wm[2 * PIECES + n, :, pl.ds(pl.multiple_of(theirs * SUB, SUB), SUB)])[:ROWS].astype(BF16)
        t3[n] = dot(hid[...], wm[2 * PIECES + n, :, pl.ds(pl.multiple_of(own * SUB, SUB), SUB)])[:ROWS]
        second_a(n).start()

    def cross(n):
        second_a(n).wait_recv()
        a2[n] = (t3[n] + r2[n].astype(F32)).astype(BF16)
        second_b(n).start()

    for n in range(PIECES):
        down(n)
        if n >= 1:
            cross(n - 1)
    cross(PIECES - 1)
    for n in range(PIECES):
        second_b(n).wait_recv()
        off = pl.multiple_of(n % 2 * NCOL + own * SUB, SUB)
        mine = hb[n // 2, :, :, pl.ds(off, SUB)].astype(F32).reshape(ROWS, SUB)
        y[:, cols_of(n)] = (mine + (a2[n].astype(F32) + b2[n].astype(F32))).astype(BF16)
        second_c(n).start()
    for n in range(PIECES):
        second_c(n).wait()
        second_a(n).wait_send()
        second_b(n).wait_send()


def layer(x, k_cache, v_cache, gain_a, wq, wo, gain_m, w_gate, w_up, w_down):
    hbm = pl.BlockSpec(memory_space=pl.ANY)
    vmem, dma = pltpu.VMEM, pltpu.SemaphoreType.DMA
    return pl.pallas_call(
        kernel,
        out_shape=pltpu.VMEM((ROWS, D), BF16),
        in_specs=[hbm] * 11,
        out_specs=pl.BlockSpec(memory_space=pltpu.VMEM),
        scratch_shapes=[
            vmem((CHUNKS, CHUNK, D), BF16),
            vmem((D // 128, 128), BF16),
            vmem((D // 128, 128), BF16),
            vmem((8, HEAD), F32),
            vmem((D, HEADS * HEAD), BF16),
            vmem((HEADS * HEAD, D), BF16),
            vmem((3 * PIECES, D, NCOL), BF16),
            vmem((DEPTH, 2, KV, HEAD), BF16),
            vmem((DEPTH, 2, KV, HEAD), BF16),
            vmem((ROWS, HEADS * HEAD), F32),
            vmem((8, KV), F32),
            vmem((PAIRS, 8, 2 * HEAD), F32),
            vmem((TALL, D), BF16),
            vmem((TALL, FF), BF16),
            vmem((CHUNKS, 2, CHUNK, HALF), BF16),
            vmem((2, CHUNKS, CHUNK, HALF), BF16),
            vmem((CHUNKS, 3, 2, CHUNK, HALF), BF16),
            vmem((CHUNKS, CHUNK, D), F32),
            vmem((PIECES, ROWS, SUB), BF16),
            vmem((PIECES, ROWS, SUB), F32),
            vmem((PIECES, ROWS, SUB), BF16),
            vmem((PIECES, ROWS, SUB), BF16),
            vmem((PIECES, ROWS, SUB), BF16),
            dma((6,)),
            dma((DEPTH,)),
            dma((DEPTH,)),
            dma((3 * PIECES,)),
            dma((2, 3, CHUNKS)),
            dma((3, 2, PIECES)),
        ],
        compiler_params=pltpu.CompilerParams(collective_id=0, has_side_effects=True, vmem_limit_bytes=62000000),
    )(
        x.reshape(CHUNKS, CHUNK, D),
        k_cache.reshape(CHUNKS, 2, PER, KV, HEAD),
        v_cache.reshape(CHUNKS, 2, PER, KV, HEAD),
        gain_a.reshape(D // 128, 128),
        wq,
        wo,
        gain_m.reshape(D // 128, 128),
        w_gate,
        w_up,
        w_down,
        jnp.asarray(rope_table()),
    )


def solution(mesh):
    states, cache, columns, rows_of = P("dp", None), P("dp", None, "tp", None), P(None, "tp"), P("tp", None)
    return jax.shard_map(
        layer,
        mesh=mesh,
        in_specs=(states, cache, cache, P(None), columns, rows_of, P(None), columns, columns, rows_of),
        out_specs=states,
        check_vma=False,
    )
```
